32 devices in a mesh: prow: 4 (over y, core), pcol: 8 (over z, x).
Axes of the slice: x: 2, y: 2, z: 4, core: 2. Of those that a mesh axis runs over, the one named last changes fastest.
Arguments:
- vectors: bfloat16 [512, 120064], P('pcol', 'prow'), may hold values from -6 to 6
- reflectors: bfloat16 [2, 256, 120064], P(None, 'pcol', 'prow'), may hold values from -6 to 6
- panel_factor: float32 [2, 256, 256], replicated, as said below
Outputs:
- band_vectors: bfloat16 [8, 64, 120064], P('pcol', 'prow')
The draws below stay inside these ranges and needn't reach their ends.
Inputs may be any that keep to these rules, and one draw needn't show every extreme that they name: `panel_factor`: upper triangular: zero below the diagonal; diagonal entries between 1 / 120064 and 3 / 120064.
All inputs are finite; a program needn't handle non-finite values.
Results may differ from the reference program's by a relative error of at most 0.0095.
Values may be sent and summed in bfloat16 or wider, within the bound.
A program may use at most 192 MiB of HBM per device.

```python
import jax
import jax.numpy as jnp
from jax import lax

ORDER = 120064
PANEL = 256
PANELS = 2
COLS_DEV = 64
NEV = 512
N_PCOL = 8


def draw_panel_factor(key, part):
    first_key, second_key = jax.random.split(jax.random.fold_in(key, 7))
    shape = (PANELS, PANEL, PANEL)
    upper_part = jax.random.normal(first_key, shape, jnp.float32) * (0.6 / ORDER)
    diag_part = jax.random.uniform(second_key, (PANELS, PANEL), jnp.float32, 1.0, 3.0) / ORDER
    row_ids = lax.broadcasted_iota(jnp.int32, shape, 1)
    col_ids = lax.broadcasted_iota(jnp.int32, shape, 2)
    result = jnp.where(col_ids > row_ids, upper_part, 0.0)
    result = result + jnp.where(col_ids == row_ids, diag_part[:, :, None], 0.0)
    return result.astype(jnp.float32)


def shard_levels(own_key, dims, pieces, low, top_value):
    factor_of = 1.0
    for position, blocks in pieces:
        steps = jax.random.uniform(jax.random.fold_in(jax.random.fold_in(own_key, 6), position), (blocks,), jnp.float32, low / len(pieces), top_value / len(pieces))
        factor_of = factor_of * jnp.repeat(jnp.exp(steps), dims[position] // blocks).reshape((-1,) + (1,) * (len(dims) - 1 - position))
    return factor_of


def scatter_about(rng, shape, deviation, most, cuts=(), dtype=jnp.bfloat16):
    entries = deviation * jax.random.normal(rng, shape, jnp.float32)
    if cuts:
        entries = entries * shard_levels(rng, shape, cuts, -0.22, 0.18)
    return jnp.clip(entries, -most, most).astype(dtype)


def setup_inputs(seed: int = 0) -> dict:
    streams_of = jax.random.split(jax.random.key(seed), 4)
    vectors = scatter_about(streams_of[0], (NEV, ORDER), 1.0, 6.0, ((0, 8), (1, 4)))
    reflectors = scatter_about(streams_of[1], (PANELS, PANEL, ORDER), 1.0, 6.0, ((1, 8), (2, 4)))
    panel_factor = draw_panel_factor(jax.random.fold_in(streams_of[3], 71), 0)
    return dict(vectors=vectors, reflectors=reflectors, panel_factor=panel_factor)


def apply_panel(current, panel, factor):
    projected = lax.dot_general(current, panel, (((1,), (1,)), ((), ())), preferred_element_type=jnp.float32)
    scaled = lax.dot_general(projected, factor, (((1,), (1,)), ((), ())), precision=lax.Precision.HIGHEST, preferred_element_type=jnp.float32).astype(jnp.bfloat16)
    updated = current.astype(jnp.float32) - jnp.dot(scaled, panel, preferred_element_type=jnp.float32)
    return updated.astype(jnp.bfloat16)


def reference(vectors, reflectors, panel_factor):
    current = vectors
    for number in range(PANELS):
        current = apply_panel(current, reflectors[number], panel_factor[number])
    return current.reshape(N_PCOL, COLS_DEV, ORDER)
```

```python
import functools

import jax
import jax.numpy as jnp
from jax import lax
from jax.experimental import pallas as pl
from jax.experimental.pallas import tpu as pltpu
from jax.sharding import PartitionSpec as P

MESH = pl.DeviceIdType.MESH
LANES = 128
SPLIT = 4
F32, BF16 = jnp.float32, jnp.bfloat16
NT = (((1,), (1,)), ((), ()))


def kernel(
    n_row, n_col, chunk, k_block, out_blocks,
    v_ref, w_ref, t_ref, o_ref,
    v_s, w_s, part, rs_send, rs_recv, ag, s_s,
    v_send, v_recv, w_send, w_recv, r_send, r_recv, g_send, g_recv, o_send, o_recv, l_sem,
):
    me_r, me_c = lax.axis_index("prow"), lax.axis_index("pcol")
    me_a, me_b = lax.rem(me_c, SPLIT), lax.div(me_c, SPLIT)
    halves, group = n_col // SPLIT, SPLIT * n_row
    me_g = me_a * n_row + me_r
    width = v_s.shape[2]
    rows = SPLIT * v_s.shape[1]
    panel = w_s.shape[1] * w_s.shape[2]
    own = v_s.shape[1] // n_row

    def remote(src, dst, send, recv, r, c):
        return pltpu.make_async_remote_copy(
            src_ref=src, dst_ref=dst, send_sem=send, recv_sem=recv,
            device_id={"prow": r, "pcol": c}, device_id_type=MESH,
        )

    def cut(ref_rows, q):
        return ref_rows.at[:, pl.ds(pl.multiple_of(q * chunk, LANES), chunk)]

    def cut_w(q):
        return w_ref.at[:, :, pl.ds(pl.multiple_of(q * chunk, LANES), chunk)]

    def slot_w(c):
        return w_s.at[:, c, :, pl.ds(0, chunk)]

    def slot_v(a):
        return v_s.at[a, :, pl.ds(0, chunk)]

    sends, arrivals, local = [], [], []
    for kb in reversed(range(halves)):
        b = lax.rem(me_b + kb, halves)
        for ka in reversed(range(SPLIT)):
            q = lax.rem(me_a + ka, SPLIT)
            c = b * SPLIT + q
            if ka or kb:
                copy = remote(cut_w(q), slot_w(me_c), w_send.at[c], w_recv.at[me_c], me_r, c)
                copy.start()
                sends.append(copy)
                arrivals.append(
                    remote(cut_w(q), slot_w(c), w_send.at[c], w_recv.at[c], me_r, c)
                )
            else:
                copy = pltpu.make_async_copy(cut_w(me_a), slot_w(me_c), l_sem.at[0])
                copy.start()
                local.append(copy)
            if kb == 0:
                if ka:
                    copy = remote(cut(v_ref, q), slot_v(me_a), v_send.at[q], v_recv.at[me_a], me_r, c)
                    copy.start()
                    sends.append(copy)
                    arrivals.append(
                        remote(cut(v_ref, q), slot_v(q), v_send.at[q], v_recv.at[q], me_r, c)
                    )
                else:
                    copy = pltpu.make_async_copy(cut(v_ref, me_a), slot_v(me_a), l_sem.at[1])
                    copy.start()
                    local.append(copy)
    if width > chunk:
        v_s[:, :, chunk:] = jnp.zeros((SPLIT, v_s.shape[1], width - chunk), BF16)
        w_s[:, :, :, chunk:] = jnp.zeros((2, n_col, w_s.shape[2], width - chunk), BF16)
    part[...] = jnp.zeros_like(part)
    for copy in local:
        copy.wait()
    for copy in arrivals:
        copy.wait_recv()

    def panel_of(p, cols):
        block = w_s[p, :, :, cols]
        if w_s.shape[2] % 16:
            block = block.astype(F32)
        return block.reshape(panel, block.shape[-1]).astype(BF16)

    @pl.loop(0, width // k_block)
    def _(i):
        cols = pl.ds(pl.multiple_of(i * k_block, k_block), k_block)
        v = v_s[:, :, cols].reshape(rows, k_block)
        first, second = panel_of(0, cols), panel_of(1, cols)
        part[:, :panel] += lax.dot_general(v, first, NT, preferred_element_type=F32)
        part[:, panel:2 * panel] += lax.dot_general(v, second, NT, preferred_element_type=F32)
        part[:, 2 * panel:] += lax.dot_general(first, second, NT, preferred_element_type=F32)

    rs_send[...] = part[...].astype(BF16).reshape(rs_send.shape)
    partners = [lax.rem(me_g + k, group) for k in range(1, group)]

    def place(g):
        return lax.rem(g, n_row), me_b * SPLIT + lax.div(g, n_row)

    got = []
    for g in partners:
        copy = remote(rs_send.at[g], rs_recv.at[me_g], r_send.at[g], r_recv.at[me_g], *place(g))
        copy.start()
        sends.append(copy)
        got.append(remote(rs_send.at[g], rs_recv.at[g], r_send.at[g], r_recv.at[g], *place(g)))
    total = rs_send[me_g].astype(F32)
    for g, copy in zip(partners, got):
        copy.wait_recv()
        total += rs_recv[g].astype(F32)
    ag[me_g] = total.astype(BF16)
    got = []
    for g in partners:
        copy = remote(ag.at[me_g], ag.at[me_g], g_send.at[g], g_recv.at[me_g], *place(g))
        copy.start()
        sends.append(copy)
        got.append(remote(ag.at[me_g], ag.at[g], g_send.at[g], g_recv.at[g], *place(g)))
    for copy in got:
        copy.wait_recv()

    sums = ag[...].reshape(rows, 3 * panel)
    high = lax.Precision.HIGHEST
    s1 = lax.dot_general(
        sums[:, :panel].astype(F32), t_ref[0], NT, precision=high, preferred_element_type=F32
    ).astype(BF16)
    p2 = sums[:, panel:2 * panel].astype(F32) - jnp.dot(
        s1, sums[:, 2 * panel:], preferred_element_type=F32
    )
    s2 = lax.dot_general(p2, t_ref[1], NT, precision=high, preferred_element_type=F32).astype(BF16)
    s_s[0] = s1
    s_s[1] = s2

    n_block = 2 * LANES
    got = []
    for j, (start, stop) in enumerate(out_blocks):
        size = min(stop, chunk) - start

        @pl.loop(start // n_block, stop // n_block)
        def _(i):
            cols = pl.ds(pl.multiple_of(i * n_block, n_block), n_block)
            v = v_s[:, :, cols].reshape(rows, n_block).astype(F32)
            v = v - jnp.dot(s_s[0], panel_of(0, cols), preferred_element_type=F32)
            v = v - jnp.dot(s_s[1], panel_of(1, cols), preferred_element_type=F32)
            v_s[:, :, cols] = v.astype(BF16).reshape(SPLIT, rows // SPLIT, n_block)

        def piece(g):
            r = lax.rem(g, n_row)
            return v_s.at[
                lax.div(g, n_row), pl.ds(pl.multiple_of(r * own, own), own), pl.ds(start, size)
            ]

        def landing(g):
            at = pl.multiple_of(lax.div(g, n_row) * chunk + start, LANES)
            return o_ref.at[lax.rem(g, n_row), :, pl.ds(at, size)]

        for g in partners:
            copy = remote(piece(g), landing(me_g), o_send.at[g, j], o_recv.at[me_g, j], *place(g))
            copy.start()
            sends.append(copy)
            got.append(remote(piece(g), landing(g), o_send.at[g, j], o_recv.at[g, j], *place(g)))
        copy = pltpu.make_async_copy(piece(me_g), landing(me_g), o_send.at[me_g, j])
        copy.start()
        got.append(copy)
    for copy in got:
        if hasattr(copy, "wait_recv") and copy.is_remote:
            copy.wait_recv()
        else:
            copy.wait()
    for copy in sends:
        copy.wait_send()


def shifted(x, offsets, mine, width):
    result = None
    for offset in sorted(set(offsets)):
        pads = [(0, 0)] * (x.ndim - 1) + [(offset, width - offset - x.shape[-1])]
        moved = jnp.pad(x, pads)
        result = moved if result is None else jnp.where(mine == offset, moved, result)
    return result


def assemble(received, columns):
    n_row = received.shape[0]
    pieces = []
    for r in range(n_row):
        low, high = r * columns, (r + 1) * columns
        first, last = low // LANES, -(-high // LANES)
        begin = 1 if low % LANES else 0
        shared = bool(high % LANES) and r + 1 < n_row
        end = last - first - (1 if shared else 0)
        stop = end * LANES if r + 1 < n_row else high - first * LANES
        pieces.append(received[r, :, begin * LANES:stop])
        if shared:
            pieces.append(
                received[r, :, end * LANES:(end + 1) * LANES] + received[r + 1, :, :LANES]
            )
    return jnp.concatenate(pieces, axis=1)


def body(n_row, n_col, vectors, reflectors, panel_factor):
    own_rows, columns = vectors.shape
    panel = panel_factor.shape[1]
    offsets = [r * columns % LANES for r in range(n_row)]
    chunk = -(-(columns + max(offsets)) // (SPLIT * LANES)) * LANES
    n_block = 2 * LANES
    width = -(-chunk // n_block) * n_block
    k_block = max(k for k in (256, 512, 768) if width % k == 0)
    mine = lax.axis_index("prow") * columns % LANES
    v = shifted(vectors, offsets, mine, SPLIT * chunk)
    w = shifted(reflectors, offsets, mine, SPLIT * chunk)
    group = SPLIT * n_row
    rows = SPLIT * own_rows
    step = -(-width // n_block // 4) * n_block
    out_blocks = [(s, min(s + step, width)) for s in range(0, width, step)]
    dma = pltpu.SemaphoreType.DMA
    received = pl.pallas_call(
        functools.partial(kernel, n_row, n_col, chunk, k_block, out_blocks),
        out_shape=jax.ShapeDtypeStruct((n_row, own_rows // n_row, SPLIT * chunk), BF16),
        in_specs=[
            pl.BlockSpec(memory_space=pl.ANY),
            pl.BlockSpec(memory_space=pl.ANY),
            pl.BlockSpec(memory_space=pltpu.VMEM),
        ],
        out_specs=pl.BlockSpec(memory_space=pl.ANY),
        scratch_shapes=[
            pltpu.VMEM((SPLIT, own_rows, width), BF16),
            pltpu.VMEM((2, n_col, reflectors.shape[1], width), BF16),
            pltpu.VMEM((rows, 3 * panel), F32),
            pltpu.VMEM((group, rows // group, 3 * panel), BF16),
            pltpu.VMEM((group, rows // group, 3 * panel), BF16),
            pltpu.VMEM((group, rows // group, 3 * panel), BF16),
            pltpu.VMEM((2, rows, panel), BF16),
            dma((SPLIT,)), dma((SPLIT,)), dma((n_col,)), dma((n_col,)),
            dma((group,)), dma((group,)), dma((group,)), dma((group,)),
            dma((group, len(out_blocks))), dma((group, len(out_blocks))), dma((2,)),
        ],
        compiler_params=pltpu.CompilerParams(
            has_side_effects=True, vmem_limit_bytes=56 * 1024 * 1024
        ),
        name="panels",
    )(v, w, panel_factor)
    return assemble(received, columns)[None]


def solution(mesh):
    placed = (P("pcol", "prow"), P(None, "pcol", "prow"), P())
    return jax.shard_map(
        functools.partial(body, mesh.shape["prow"], mesh.shape["pcol"]),
        mesh=mesh, in_specs=placed, out_specs=P("pcol", "prow", None), check_vma=False,
    )
```

```python
import functools

import jax
import jax.numpy as jnp
from jax import lax
from jax.experimental import pallas as pl
from jax.experimental.pallas import tpu as pltpu
from jax.sharding import PartitionSpec as P

MESH = pl.DeviceIdType.MESH
LANES = 128
SPLIT = 4
F32, BF16 = jnp.float32, jnp.bfloat16
NT = (((1,), (1,)), ((), ()))


def kernel(
    n_row, n_col, main, k_block, out_blocks,
    v_ref, w_ref, vx_ref, wx_ref, t_ref, o_ref,
    v_s, w_s, part, rs_send, rs_recv, ag, s_s,
    v_send, v_recv, w_send, w_recv, r_send, r_recv, g_send, g_recv, o_send, o_recv, l_sem,
):
    me_r, me_c = lax.axis_index("prow"), lax.axis_index("pcol")
    me_a, me_b = lax.rem(me_c, SPLIT), lax.div(me_c, SPLIT)
    halves, group = n_col // SPLIT, SPLIT * n_row
    me_g = me_a * n_row + me_r
    width = v_s.shape[2]
    rows = SPLIT * v_s.shape[1]
    panel = w_s.shape[1] * w_s.shape[2]
    own = v_s.shape[1] // n_row
    middle = width // 2
    pieces = ((0, middle), (middle, main), (main, main + LANES))

    def remote(src, dst, send, recv, r, c):
        return pltpu.make_async_remote_copy(
            src_ref=src, dst_ref=dst, send_sem=send, recv_sem=recv,
            device_id={"prow": r, "pcol": c}, device_id_type=MESH,
        )

    def source(number, q):
        start, stop = pieces[number]
        if start == main:
            return pl.ds(pl.multiple_of(q * LANES, LANES), LANES)
        return pl.ds(pl.multiple_of(q * main + start, LANES), stop - start)

    def move(kind, number, b, q, c, here):
        start, stop = pieces[number]
        target = pl.ds(start, stop - start)
        if kind == "v":
            src = (vx_ref if start == main else v_ref).at[:, source(number, q)]
            slot, sent, come, mine, theirs = (
                lambda a: v_s.at[a, :, target], v_send, v_recv, me_a, q
            )
        else:
            src = (wx_ref if start == main else w_ref).at[:, :, source(number, q)]
            slot, sent, come, mine, theirs = (
                lambda a: w_s.at[:, a, :, target], w_send, w_recv, me_c, c
            )
        if here:
            copy = pltpu.make_async_copy(src, slot(mine), l_sem.at[number, 0 if kind == "v" else 1])
            copy.start()
            local[number].append(copy)
            return
        copy = remote(src, slot(mine), sent.at[number, theirs], come.at[number, mine], me_r, c)
        copy.start()
        sends.append(copy)
        arrivals[number].append(
            remote(src, slot(theirs), sent.at[number, theirs], come.at[number, theirs], me_r, c)
        )

    sends, arrivals, local = [], [[], [], []], [[], [], []]
    for number in (0, 2, 1):
        near, far = [], []
        for ka in reversed(range(SPLIT)):
            q = lax.rem(me_a + ka, SPLIT)
            near.append(("v", number, me_b, q, me_b * SPLIT + q, ka == 0))
            near.append(("w", number, me_b, q, me_b * SPLIT + q, ka == 0))
        for kb in reversed(range(1, halves)):
            b = lax.rem(me_b + kb, halves)
            for ka in reversed(range(SPLIT)):
                q = lax.rem(me_a + ka + 2 * me_r, SPLIT)
                far.append(("w", number, b, q, b * SPLIT + q, False))
        for at in range(max(len(near), len(far))):
            for order in (near, far):
                if at < len(order):
                    move(*order[at])
    if width > main + LANES:
        pad = width - main - LANES
        v_s[:, :, main + LANES:] = jnp.zeros((SPLIT, v_s.shape[1], pad), BF16)
        w_s[:, :, :, main + LANES:] = jnp.zeros((2, n_col, w_s.shape[2], pad), BF16)
    part[...] = jnp.zeros_like(part)

    def panel_of(p, cols):
        block = w_s[p, :, :, cols]
        if w_s.shape[2] % 16:
            block = block.astype(F32)
        return block.reshape(panel, block.shape[-1]).astype(BF16)

    def products(begin, end):
        @pl.loop(begin // k_block, end // k_block)
        def _(i):
            cols = pl.ds(pl.multiple_of(i * k_block, k_block), k_block)
            v = v_s[:, :, cols].reshape(rows, k_block)
            first, second = panel_of(0, cols), panel_of(1, cols)
            part[:, :panel] += lax.dot_general(v, first, NT, preferred_element_type=F32)
            part[:, panel:2 * panel] += lax.dot_general(v, second, NT, preferred_element_type=F32)
            part[:, 2 * panel:] += lax.dot_general(first, second, NT, preferred_element_type=F32)

    def landed(number):
        for copy in local[number]:
            copy.wait()
        for copy in arrivals[number]:
            copy.wait_recv()

    landed(0)
    products(0, middle)
    landed(2)
    landed(1)
    products(middle, width)

    rs_send[...] = part[...].astype(BF16).reshape(rs_send.shape)
    partners = [lax.rem(me_g + k, group) for k in range(1, group)]

    def place(g):
        return lax.rem(g, n_row), me_b * SPLIT + lax.div(g, n_row)

    got = []
    for g in partners:
        copy = remote(rs_send.at[g], rs_recv.at[me_g], r_send.at[g], r_recv.at[me_g], *place(g))
        copy.start()
        sends.append(copy)
        got.append(remote(rs_send.at[g], rs_recv.at[g], r_send.at[g], r_recv.at[g], *place(g)))
    total = rs_send[me_g].astype(F32)
    for g, copy in zip(partners, got):
        copy.wait_recv()
        total += rs_recv[g].astype(F32)
    ag[me_g] = total.astype(BF16)
    got = []
    for g in partners:
        copy = remote(ag.at[me_g], ag.at[me_g], g_send.at[g], g_recv.at[me_g], *place(g))
        copy.start()
        sends.append(copy)
        got.append(remote(ag.at[me_g], ag.at[g], g_send.at[g], g_recv.at[g], *place(g)))
    for copy in got:
        copy.wait_recv()

    sums = ag[...].reshape(rows, 3 * panel)
    high = lax.Precision.HIGHEST
    s1 = lax.dot_general(
        sums[:, :panel].astype(F32), t_ref[0], NT, precision=high, preferred_element_type=F32
    ).astype(BF16)
    p2 = sums[:, panel:2 * panel].astype(F32) - jnp.dot(
        s1, sums[:, 2 * panel:], preferred_element_type=F32
    )
    s2 = lax.dot_general(p2, t_ref[1], NT, precision=high, preferred_element_type=F32).astype(BF16)
    s_s[0] = s1
    s_s[1] = s2

    n_block = 2 * LANES
    got = []

    def hand_out(j, start, size):
        def piece(g):
            r = lax.rem(g, n_row)
            return v_s.at[
                lax.div(g, n_row), pl.ds(pl.multiple_of(r * own, own), own), pl.ds(start, size)
            ]

        def landing(g):
            a = lax.div(g, n_row)
            at = SPLIT * main + a * LANES if start == main else a * main + start
            return o_ref.at[lax.rem(g, n_row), :, pl.ds(pl.multiple_of(at, LANES), size)]

        for g in partners:
            copy = remote(piece(g), landing(me_g), o_send.at[g, j], o_recv.at[me_g, j], *place(g))
            copy.start()
            sends.append(copy)
            got.append(
                remote(piece(g), landing(g), o_send.at[g, j], o_recv.at[g, j], *place(g)).wait_recv
            )
        copy = pltpu.make_async_copy(piece(me_g), landing(me_g), o_send.at[me_g, j])
        copy.start()
        got.append(copy.wait)

    for j, (start, stop) in enumerate(out_blocks):

        @pl.loop(start // n_block, stop // n_block)
        def _(i):
            cols = pl.ds(pl.multiple_of(i * n_block, n_block), n_block)
            v = v_s[:, :, cols].reshape(rows, n_block).astype(F32)
            v = v - jnp.dot(s_s[0], panel_of(0, cols), preferred_element_type=F32)
            v = v - jnp.dot(s_s[1], panel_of(1, cols), preferred_element_type=F32)
            v_s[:, :, cols] = v.astype(BF16).reshape(SPLIT, rows // SPLIT, n_block)

        hand_out(j, start, min(stop, main) - start)
        if stop > main:
            hand_out(len(out_blocks), main, LANES)
    for wait in got:
        wait()
    for copy in sends:
        copy.wait_send()


def lay_out(columns, in_ref, out_ref):
    for r in range(in_ref.shape[0]):
        out_ref[:, r * columns:(r + 1) * columns] = in_ref[r, :, :columns]


def body(n_row, n_col, vectors, reflectors, panel_factor):
    own_rows, columns = vectors.shape
    panel = panel_factor.shape[1]
    main = columns // (SPLIT * LANES) * LANES
    covered = SPLIT * main
    k_block = 6 * LANES
    width = -(-(main + LANES) // (2 * k_block)) * 2 * k_block
    n_block = 2 * LANES
    extra = SPLIT * LANES - (columns - covered)
    v_x = jnp.pad(vectors[:, covered:], ((0, 0), (0, extra)))
    w_x = jnp.pad(reflectors[:, :, covered:], ((0, 0), (0, 0), (0, extra)))
    group = SPLIT * n_row
    rows = SPLIT * own_rows
    step = -(-width // n_block // 4) * n_block
    out_blocks = [(s, min(s + step, width)) for s in range(0, width, step)]
    out_count = len(out_blocks) + 1
    dma = pltpu.SemaphoreType.DMA
    received = pl.pallas_call(
        functools.partial(kernel, n_row, n_col, main, k_block, out_blocks),
        out_shape=jax.ShapeDtypeStruct(
            (n_row, own_rows // n_row, covered + SPLIT * LANES), BF16
        ),
        in_specs=[pl.BlockSpec(memory_space=pl.ANY)] * 4
        + [pl.BlockSpec(memory_space=pltpu.VMEM)],
        out_specs=pl.BlockSpec(memory_space=pl.ANY),
        scratch_shapes=[
            pltpu.VMEM((SPLIT, own_rows, width), BF16),
            pltpu.VMEM((2, n_col, reflectors.shape[1], width), BF16),
            pltpu.VMEM((rows, 3 * panel), F32),
            pltpu.VMEM((group, rows // group, 3 * panel), BF16),
            pltpu.VMEM((group, rows // group, 3 * panel), BF16),
            pltpu.VMEM((group, rows // group, 3 * panel), BF16),
            pltpu.VMEM((2, rows, panel), BF16),
            dma((3, SPLIT)), dma((3, SPLIT)), dma((3, n_col)), dma((3, n_col)),
            dma((group,)), dma((group,)), dma((group,)), dma((group,)),
            dma((group, out_count)), dma((group, out_count)), dma((3, 2)),
        ],
        compiler_params=pltpu.CompilerParams(
            has_side_effects=True, vmem_limit_bytes=56 * 1024 * 1024
        ),
        name="panels",
    )(vectors, reflectors, v_x, w_x, panel_factor)
    whole = pl.pallas_call(
        functools.partial(lay_out, columns),
        out_shape=jax.ShapeDtypeStruct((own_rows // n_row, n_row * columns), BF16),
        in_specs=[pl.BlockSpec(memory_space=pltpu.VMEM)],
        out_specs=pl.BlockSpec(memory_space=pltpu.VMEM),
        compiler_params=pltpu.CompilerParams(vmem_limit_bytes=24 * 1024 * 1024),
        name="lay_out",
    )(received)
    return whole[None]


def solution(mesh):
    placed = (P("pcol", "prow"), P(None, "pcol", "prow"), P())
    return jax.shard_map(
        functools.partial(body, mesh.shape["prow"], mesh.shape["pcol"]),
        mesh=mesh, in_specs=placed, out_specs=P("pcol", "prow", None), check_vma=False,
    )
```

```python
import functools

import jax
import jax.numpy as jnp
from jax import lax
from jax.experimental import pallas as pl
from jax.experimental.pallas import tpu as pltpu
from jax.sharding import PartitionSpec as P

MESH = pl.DeviceIdType.MESH
LANES = 128
SPLIT = 4
F32, BF16 = jnp.float32, jnp.bfloat16
NT = (((1,), (1,)), ((), ()))


def kernel(
    n_row, n_col, main, k_block, out_blocks,
    v_ref, w_ref, vx_ref, wx_ref, t_ref, o_ref,
    v_s, w_s, part, rs_send, rs_recv, ag, s_s,
    v_send, v_recv, w_send, w_recv, r_send, r_recv, g_send, g_recv, o_send, o_recv, l_sem,
):
    me_r, me_c = lax.axis_index("prow"), lax.axis_index("pcol")
    me_a, me_b = lax.rem(me_c, SPLIT), lax.div(me_c, SPLIT)
    halves, group = n_col // SPLIT, SPLIT * n_row
    me_g = me_a * n_row + me_r
    width = v_s.shape[2]
    rows = SPLIT * v_s.shape[1]
    panel = w_s.shape[1] * w_s.shape[2]
    own = v_s.shape[1] // n_row
    middle = width // 2
    pieces = ((0, middle), (middle, main), (main, main + LANES))

    def remote(src, dst, send, recv, r, c):
        return pltpu.make_async_remote_copy(
            src_ref=src, dst_ref=dst, send_sem=send, recv_sem=recv,
            device_id={"prow": r, "pcol": c}, device_id_type=MESH,
        )

    def source(number, q):
        start, stop = pieces[number]
        if start == main:
            return pl.ds(pl.multiple_of(q * LANES, LANES), LANES)
        return pl.ds(pl.multiple_of(q * main + start, LANES), stop - start)

    def move(kind, number, b, q, c, here):
        start, stop = pieces[number]
        target = pl.ds(start, stop - start)
        if kind == "v":
            src = (vx_ref if start == main else v_ref).at[:, source(number, q)]
            slot, sent, come, mine, theirs = (
                lambda a: v_s.at[a, :, target], v_send, v_recv, me_a, q
            )
        else:
            src = (wx_ref if start == main else w_ref).at[:, :, source(number, q)]
            slot, sent, come, mine, theirs = (
                lambda a: w_s.at[:, a, :, target], w_send, w_recv, me_c, c
            )
        if here:
            copy = pltpu.make_async_copy(src, slot(mine), l_sem.at[number, 0 if kind == "v" else 1])
            copy.start()
            local[number].append(copy)
            return
        copy = remote(src, slot(mine), sent.at[number, theirs], come.at[number, mine], me_r, c)
        copy.start()
        sends.append(copy)
        arrivals[number].append(
            remote(src, slot(theirs), sent.at[number, theirs], come.at[number, theirs], me_r, c)
        )

    sends, arrivals, local = [], [[], [], []], [[], [], []]
    for number in (0, 2, 1):
        near, far = [], []
        for ka in reversed(range(SPLIT)):
            q = lax.rem(me_a + ka, SPLIT)
            near.append(("v", number, me_b, q, me_b * SPLIT + q, ka == 0))
            near.append(("w", number, me_b, q, me_b * SPLIT + q, ka == 0))
        for kb in reversed(range(1, halves)):
            b = lax.rem(me_b + kb, halves)
            for ka in reversed(range(SPLIT)):
                q = lax.rem(me_a + ka + 2 * me_r, SPLIT)
                far.append(("w", number, b, q, b * SPLIT + q, False))
        for at in range(max(len(near), len(far))):
            for order in (near, far):
                if at < len(order):
                    move(*order[at])
    if width > main + LANES:
        pad = width - main - LANES
        v_s[:, :, main + LANES:] = jnp.zeros((SPLIT, v_s.shape[1], pad), BF16)
        w_s[:, :, :, main + LANES:] = jnp.zeros((2, n_col, w_s.shape[2], pad), BF16)
    part[...] = jnp.zeros_like(part)

    def panel_of(p, cols):
        block = w_s[p, :, :, cols]
        if w_s.shape[2] % 16:
            block = block.astype(F32)
        return block.reshape(panel, block.shape[-1]).astype(BF16)

    def products(begin, end):
        @pl.loop(begin // k_block, end // k_block)
        def _(i):
            cols = pl.ds(pl.multiple_of(i * k_block, k_block), k_block)
            v = v_s[:, :, cols].reshape(rows, k_block)
            first, second = panel_of(0, cols), panel_of(1, cols)
            part[:, :panel] += lax.dot_general(v, first, NT, preferred_element_type=F32)
            part[:, panel:2 * panel] += lax.dot_general(v, second, NT, preferred_element_type=F32)
            part[:, 2 * panel:] += lax.dot_general(first, second, NT, preferred_element_type=F32)

    def landed(number):
        for copy in local[number]:
            copy.wait()
        for copy in arrivals[number]:
            copy.wait_recv()

    landed(0)
    products(0, middle)
    landed(2)
    landed(1)
    products(middle, width)

    rs_send[...] = part[...].astype(BF16).reshape(rs_send.shape)
    partners = [lax.rem(me_g + k, group) for k in range(1, group)]

    def place(g):
        return lax.rem(g, n_row), me_b * SPLIT + lax.div(g, n_row)

    got = []
    for g in partners:
        copy = remote(rs_send.at[g], rs_recv.at[me_g], r_send.at[g], r_recv.at[me_g], *place(g))
        copy.start()
        sends.append(copy)
        got.append(remote(rs_send.at[g], rs_recv.at[g], r_send.at[g], r_recv.at[g], *place(g)))
    total = rs_send[me_g].astype(F32)
    for g, copy in zip(partners, got):
        copy.wait_recv()
        total += rs_recv[g].astype(F32)
    ag[me_g] = total.astype(BF16)
    got = []
    for g in partners:
        copy = remote(ag.at[me_g], ag.at[me_g], g_send.at[g], g_recv.at[me_g], *place(g))
        copy.start()
        sends.append(copy)
        got.append(remote(ag.at[me_g], ag.at[g], g_send.at[g], g_recv.at[g], *place(g)))
    for copy in got:
        copy.wait_recv()

    sums = ag[...].reshape(rows, 3 * panel)
    high = lax.Precision.HIGHEST
    s1 = lax.dot_general(
        sums[:, :panel].astype(F32), t_ref[0], NT, precision=high, preferred_element_type=F32
    ).astype(BF16)
    p2 = sums[:, panel:2 * panel].astype(F32) - jnp.dot(
        s1, sums[:, 2 * panel:], preferred_element_type=F32
    )
    s2 = lax.dot_general(p2, t_ref[1], NT, precision=high, preferred_element_type=F32).astype(BF16)
    s_s[0] = s1
    s_s[1] = s2

    n_block = 2 * LANES
    got = []

    def hand_out(j, start, size):
        def piece(g):
            r = lax.rem(g, n_row)
            return v_s.at[
                lax.div(g, n_row), pl.ds(pl.multiple_of(r * own, own), own), pl.ds(start, size)
            ]

        def landing(g):
            a = lax.div(g, n_row)
            at = SPLIT * main + a * LANES if start == main else a * main + start
            return o_ref.at[lax.rem(g, n_row), :, pl.ds(pl.multiple_of(at, LANES), size)]

        for g in partners:
            copy = remote(piece(g), landing(me_g), o_send.at[g, j], o_recv.at[me_g, j], *place(g))
            copy.start()
            sends.append(copy)
            got.append(
                remote(piece(g), landing(g), o_send.at[g, j], o_recv.at[g, j], *place(g)).wait_recv
            )
        copy = pltpu.make_async_copy(piece(me_g), landing(me_g), o_send.at[me_g, j])
        copy.start()
        got.append(copy.wait)

    for j, (start, stop) in enumerate(out_blocks):

        @pl.loop(start // n_block, stop // n_block)
        def _(i):
            cols = pl.ds(pl.multiple_of(i * n_block, n_block), n_block)
            v = v_s[:, :, cols].reshape(rows, n_block).astype(F32)
            v = v - jnp.dot(s_s[0], panel_of(0, cols), preferred_element_type=F32)
            v = v - jnp.dot(s_s[1], panel_of(1, cols), preferred_element_type=F32)
            v_s[:, :, cols] = v.astype(BF16).reshape(SPLIT, rows // SPLIT, n_block)

        hand_out(j, start, min(stop, main) - start)
        if stop > main:
            hand_out(len(out_blocks), main, LANES)
    for wait in got:
        wait()
    for copy in sends:
        copy.wait_send()


def lay_out(columns, in_ref, out_ref):
    for r in range(in_ref.shape[0]):
        out_ref[:, r * columns:(r + 1) * columns] = in_ref[r, :, :columns]


def body(n_row, n_col, vectors, reflectors, panel_factor):
    own_rows, columns = vectors.shape
    panel = panel_factor.shape[1]
    main = columns // (SPLIT * LANES) * LANES
    covered = SPLIT * main
    k_block = 6 * LANES
    width = -(-(main + LANES) // (2 * k_block)) * 2 * k_block
    n_block = 2 * LANES
    extra = SPLIT * LANES - (columns - covered)
    v_x = jnp.pad(vectors[:, covered:], ((0, 0), (0, extra)))
    w_x = jnp.pad(reflectors[:, :, covered:], ((0, 0), (0, 0), (0, extra)))
    group = SPLIT * n_row
    rows = SPLIT * own_rows
    step = -(-width // n_block // 6) * n_block
    out_blocks = [(s, min(s + step, width)) for s in range(0, width, step)]
    out_count = len(out_blocks) + 1
    dma = pltpu.SemaphoreType.DMA
    received = pl.pallas_call(
        functools.partial(kernel, n_row, n_col, main, k_block, out_blocks),
        out_shape=jax.ShapeDtypeStruct(
            (n_row, own_rows // n_row, covered + SPLIT * LANES), BF16
        ),
        in_specs=[pl.BlockSpec(memory_space=pl.ANY)] * 4
        + [pl.BlockSpec(memory_space=pltpu.VMEM)],
        out_specs=pl.BlockSpec(memory_space=pl.ANY),
        scratch_shapes=[
            pltpu.VMEM((SPLIT, own_rows, width), BF16),
            pltpu.VMEM((2, n_col, reflectors.shape[1], width), BF16),
            pltpu.VMEM((rows, 3 * panel), F32),
            pltpu.VMEM((group, rows // group, 3 * panel), BF16),
            pltpu.VMEM((group, rows // group, 3 * panel), BF16),
            pltpu.VMEM((group, rows // group, 3 * panel), BF16),
            pltpu.VMEM((2, rows, panel), BF16),
            dma((3, SPLIT)), dma((3, SPLIT)), dma((3, n_col)), dma((3, n_col)),
            dma((group,)), dma((group,)), dma((group,)), dma((group,)),
            dma((group, out_count)), dma((group, out_count)), dma((3, 2)),
        ],
        compiler_params=pltpu.CompilerParams(
            has_side_effects=True, vmem_limit_bytes=56 * 1024 * 1024
        ),
        name="panels",
    )(vectors, reflectors, v_x, w_x, panel_factor)
    whole = pl.pallas_call(
        functools.partial(lay_out, columns),
        out_shape=jax.ShapeDtypeStruct((own_rows // n_row, n_row * columns), BF16),
        in_specs=[pl.BlockSpec(memory_space=pltpu.VMEM)],
        out_specs=pl.BlockSpec(memory_space=pltpu.VMEM),
        compiler_params=pltpu.CompilerParams(vmem_limit_bytes=24 * 1024 * 1024),
        name="lay_out",
    )(received)
    return whole[None]


def solution(mesh):
    placed = (P("pcol", "prow"), P(None, "pcol", "prow"), P())
    return jax.shard_map(
        functools.partial(body, mesh.shape["prow"], mesh.shape["pcol"]),
        mesh=mesh, in_specs=placed, out_specs=P("pcol", "prow", None), check_vma=False,
    )
```
